32 devices in a mesh: expert: 4 (over y, x), rep: 4 (over z), hid: 2 (over core).
Axes of the slice: x: 2, y: 2, z: 4, core: 2. Of those that a mesh axis runs over, the one named last changes fastest.
Arguments:
- calib_rows: bfloat16 [8192, 6144], P(('expert', 'rep'), 'hid'), may hold values from -6 to 6
- routes: int32 [8192, 2], P(('expert', 'rep')), may hold values from 0 to 7, all different within a row; in each aligned block of 512 rows (0 to 511, 512 to 1023, ...) at most 256 rows name the same one
- sketch_seed: int32 [6144, 512], P('hid'), may hold values from -1 to 1
- up_weight: bfloat16 [8, 6144, 16384], P('expert', 'hid', 'rep'), may hold values from -0.078125 to 0.078125
Outputs:
- projected: float32 [16384, 8, 512], P(('rep', 'hid'), 'expert')
The draws below stay inside these ranges and needn't reach their ends.
Inputs may be any that keep to these rules, and one draw needn't show every extreme that they name: `routes`: each row names 2 different experts. In each aligned block of 512 rows no expert is named by more than 256 rows, and every expert is named somewhere.
All inputs are finite; a program needn't handle non-finite values.
Results may differ from the reference program's by a relative error of at most 0.0037.
Values may be sent and summed in bfloat16 or wider, within the bound.
No kernel may reach another device: no remote copies, remote signals or barrier semaphores. Data moves between devices by JAX's collectives and lax.ppermute only.
A program may use at most 192 MiB of HBM per device.

```python
import math
import jax
import jax.numpy as jnp
import numpy as np
from jax import lax

D = 6144
FF = 16384
EXPERTS = 8
TOP = 2
R = 512
TOK_DEV = 512
CAP = 256
TOKENS = 8192


def touch_ends(result, key, smallest, largest):
    dims = result.shape
    index_at = [jax.random.randint(jax.random.fold_in(key, axis), (), 0, dims[axis]) for axis in range(len(dims))]
    result = result.at[tuple(index_at)].set(smallest)
    longest = dims.index(max(dims))
    index_at[longest] = (index_at[longest] + 1) % dims[longest]
    return result.at[tuple(index_at)].set(largest)


def shard_levels(stream_key, extent, shards, smallest, high):
    gain = 1.0
    for axis_at, shards_of in shards:
        heights = jax.random.uniform(jax.random.fold_in(jax.random.fold_in(stream_key, 6), axis_at), (shards_of,), jnp.float32, smallest / len(shards), high / len(shards))
        gain = gain * jnp.repeat(jnp.exp(heights), extent[axis_at] // shards_of).reshape((-1,) + (1,) * (len(extent) - 1 - axis_at))
    return gain


def deal_out(stream_key, own, number, rows, number_of, top, bound, skew):
    ranking = jax.random.permutation(stream_key, number_of)
    crowded, usual = shares(number_of, rows * top, bound, skew, True), shares(number_of, rows * top, bound, skew, False)
    places = jnp.arange(number_of)

    def named(tallies, offset_by):
        used = int((tallies > 0).sum())
        fixed = max(1, used // 4)
        moved = fixed + (places - fixed + offset_by * (used - fixed)) % max(1, number_of - fixed)
        return jnp.zeros((number_of,), jnp.int32).at[ranking[jnp.where(places < fixed, places, moved)]].set(jnp.asarray(tallies, jnp.int32))

    tallies = jnp.where(number % 4 == 0, named(crowded, number // 4), named(usual, number - number // 4 - 1))
    mixed = jax.random.permutation(jax.random.fold_in(own, 3), number_of)
    giver, taker = mixed[0:number_of // 2 * 2:2], mixed[1:number_of // 2 * 2:2]
    room = jnp.minimum(tallies[giver] - 1, bound - tallies[taker]) // 2
    room = jnp.where((giver == ranking[0]) | (taker == ranking[0]) | (tallies[taker] == 0), 0, jnp.maximum(room, 0))
    moved = jax.random.randint(jax.random.fold_in(own, 4), (number_of // 2,), 0, 1 << 20) % (room + 1)
    tallies = tallies.at[giver].add(-moved).at[taker].add(moved)
    labels = jnp.searchsorted(jnp.cumsum(tallies), jnp.arange(rows * top), side="right").astype(jnp.int32)
    grid = labels.reshape(top, rows).T
    grid = grid[jax.random.permutation(jax.random.fold_in(own, 1), rows)]
    offset_by = jax.random.randint(jax.random.fold_in(own, 2), (rows, 1), 0, top)
    return jnp.take_along_axis(grid, (jnp.arange(top)[None, :] + offset_by) % top, axis=1)


def shares(count, total, reach, slope, full):
    loads = [(1 << 20) // math.isqrt(rank ** slope) + 1 for rank in range(1, count + 1)]
    largest = reach if full else min(reach, max(-(-total // count), total * loads[0] // sum(loads)))
    least = 1 if total - largest >= count - 1 else 0
    holding, rest = [largest] + [least] * (count - 1), total - largest - least * (count - 1)
    while rest > 0:
        free = [i for i in range(1, count) if holding[i] < largest] or [i for i in range(1, count) if holding[i] < reach]
        pool, budget = sum([loads[i] for i in free]), rest
        for i in free:
            addition = min(reach - holding[i], max(1, budget * loads[i] // pool), rest)
            holding[i] = holding[i] + addition
            rest = rest - addition
    return np.array(holding)


def scatter_about(stream_key, extent, width, most, split=(), held_as=jnp.bfloat16):
    entries = jax.random.normal(stream_key, extent, jnp.float32) * width
    if len(split) > 0:
        entries = shard_levels(stream_key, extent, split, -0.22, 0.18) * entries
    return jnp.clip(entries, min=-most, max=most).astype(held_as)


def setup_inputs(seed: int = 0) -> dict:
    key_list = jax.random.split(jax.random.key(seed), 5)
    calib_rows = scatter_about(key_list[0], (TOKENS, D), 1.0, 6.0, ((0, 16), (1, 2)))
    routes_keys = jax.random.split(jax.random.fold_in(key_list[1], 1), TOKENS // TOK_DEV)
    routes_turns = jax.random.permutation(jax.random.fold_in(key_list[1], 3), TOKENS // TOK_DEV)
    routes = jax.vmap(lambda own, number: deal_out(jax.random.fold_in(key_list[1], 2), own, number, TOK_DEV, EXPERTS, TOP, CAP, 2))(routes_keys, routes_turns).reshape((TOKENS, TOP))
    sketch_seed = touch_ends(jax.random.randint(key_list[2], (D, R), -1, 2), jax.random.fold_in(key_list[2], 1), -1, 1).astype(jnp.int32)
    up_weight = scatter_about(key_list[3], (EXPERTS, D, FF), D ** -0.5, 0.078125, ((0, 4), (1, 2), (2, 4)))
    return {"calib_rows": calib_rows, "routes": routes, "sketch_seed": sketch_seed, "up_weight": up_weight}


damping = 0.25


def reference(calib_rows, routes, sketch_seed, up_weight):
    signs_half = sketch_seed.astype(jnp.bfloat16)
    signs_full = sketch_seed.astype(jnp.float32)
    expert_ids = jnp.arange(EXPERTS, dtype=jnp.int32)
    member = jnp.sum((routes[:, :, None] == expert_ids[None, None, :]).astype(jnp.float32), axis=1)
    row_squares = jnp.sum(jnp.square(calib_rows.astype(jnp.float32)), axis=1)
    row_counts = jnp.sum(member, axis=0)
    square_sums = jnp.sum(member * row_squares[:, None], axis=0)
    sketched = jnp.dot(calib_rows, signs_half, preferred_element_type=jnp.float32)
    transposed = calib_rows.T

    def per_expert(expert):
        member_col = lax.dynamic_index_in_dim(member, expert, 1, keepdims=False)
        masked = (sketched * member_col[:, None]).astype(jnp.bfloat16)
        gram = jnp.dot(transposed, masked, preferred_element_type=jnp.float32)
        count_one = row_counts[expert]
        ridge = damping * square_sums[expert] / (count_one * D)
        sketch = (gram / count_one + ridge * signs_full).astype(jnp.bfloat16)
        weight = up_weight[expert]
        return lax.dot_general(weight, sketch, (((0,), (0,)), ((), ())), preferred_element_type=jnp.float32)

    stacked = lax.map(per_expert, expert_ids)
    return jnp.transpose(stacked, (1, 0, 2))
```

```python
import math

import jax
import jax.numpy as jnp
from jax import lax
from jax.experimental import pallas as pl
from jax.experimental.pallas import tpu as pltpu
from jax.sharding import PartitionSpec as P


D = 6144
EXPERTS = 8
EXTRA = 16
damping = 0.25


def split3(value):
    hi = lax.reduce_precision(value, 8, 7)
    mid = lax.reduce_precision(value - hi, 8, 7)
    return jnp.stack([hi, mid, value - hi - mid])


def flip_kernel(x_ref, extra_ref, p_ref, *, d):
    flipped = x_ref[...].T
    for g in range(p_ref.shape[0]):
        p_ref[g, :d, :] = flipped[g * d : (g + 1) * d, :]
        p_ref[g, d:, :] = extra_ref[...]


def flip(calib_rows, extra, chips):
    tokens, local = calib_rows.shape
    d = local // chips
    group = 128 // math.gcd(d, 128)
    if d % 16 or chips % group:
        return jnp.concatenate(
            [
                calib_rows.T.reshape(chips, d, tokens),
                jnp.broadcast_to(extra[None], (chips, EXTRA, tokens)),
            ],
            axis=1,
        )
    return pl.pallas_call(
        lambda *refs: flip_kernel(*refs, d=d),
        out_shape=jax.ShapeDtypeStruct((chips, d + EXTRA, tokens), jnp.bfloat16),
        grid=(chips // group,),
        in_specs=[
            pl.BlockSpec((tokens, group * d), lambda j: (0, j)),
            pl.BlockSpec((EXTRA, tokens), lambda j: (0, 0)),
        ],
        out_specs=pl.BlockSpec((group, d + EXTRA, tokens), lambda j: (j, 0, 0)),
        cost_estimate=pl.CostEstimate(
            flops=tokens * local, bytes_accessed=4 * tokens * local, transcendentals=0
        ),
        name="flip",
    )(calib_rows, extra)


def gram_kernel(counts_ref, ridge_ref, x_ref, m_ref, s_ref, o_ref, lhs, acc, *, which, per, d):
    step = pl.program_id(0)
    groups = o_ref.shape[0]
    sources, _, tokens = x_ref.shape
    for s in range(sources):
        x = x_ref[s, :d, :]
        for g in range(groups):
            row = d + g * per + which
            lhs[g, :, s * tokens : (s + 1) * tokens] = x * x_ref[s, row : row + 1, :]
    flat = lhs[...].reshape(groups * d, sources * tokens)
    rows = m_ref[...].reshape(sources * tokens, m_ref.shape[-1])
    part = jnp.dot(flat, rows, preferred_element_type=jnp.float32)

    @pl.when(step == 0)
    def _():
        acc[...] = part

    @pl.when(step > 0)
    def _():
        acc[...] += part

    @pl.when(step == pl.num_programs(0) - 1)
    def _():
        signs = s_ref[...].astype(jnp.float32)
        for g in range(groups):
            e = g * per + which
            total = acc[g * d : (g + 1) * d, :]
            o_ref[g] = (total / counts_ref[e] + ridge_ref[e] * signs).astype(jnp.bfloat16)


def gram(counts, ridge, received, sketched, signs, which, per):
    sources, rows, tokens = received.shape
    d = rows - EXTRA
    batch, hid, _, share, width = sketched.shape
    groups = EXPERTS // per
    return pl.pallas_call(
        lambda *refs: gram_kernel(*refs, which=which, per=per, d=d),
        out_shape=jax.ShapeDtypeStruct((groups, d, width), jnp.bfloat16),
        grid=(sources // batch,),
        in_specs=[
            pl.BlockSpec(memory_space=pltpu.SMEM),
            pl.BlockSpec(memory_space=pltpu.SMEM),
            pl.BlockSpec((batch, rows, tokens), lambda j: (j, 0, 0)),
            pl.BlockSpec((batch, hid, 1, share, width), lambda j: (0, 0, j, 0, 0)),
            pl.BlockSpec((d, width), lambda j: (0, 0)),
        ],
        out_specs=pl.BlockSpec((groups, d, width), lambda j: (0, 0, 0)),
        scratch_shapes=[
            pltpu.VMEM((groups, d, batch * tokens), jnp.bfloat16),
            pltpu.VMEM((groups * d, width), jnp.float32),
        ],
        cost_estimate=pl.CostEstimate(
            flops=2 * sources * groups * d * tokens * width,
            bytes_accessed=2 * sources * tokens * (rows + width),
            transcendentals=0,
        ),
        name="gram",
    )(counts, ridge, received, sketched, signs)


def weave_kernel(*refs):
    fresh_ref, away_ref, o_ref = refs[-3], refs[-2], refs[-1]
    done = refs[:-3]
    for k, ref in enumerate(done):
        o_ref[:, k, :] = ref[...]
    o_ref[:, len(done), :] = fresh_ref[...] + away_ref[...]


def weave(done, fresh, away):
    block, width = fresh.shape
    per = len(done) + 1
    tile = math.gcd(block, 256)
    spec = pl.BlockSpec((tile, width), lambda i: (i, 0))
    return pl.pallas_call(
        weave_kernel,
        out_shape=jax.ShapeDtypeStruct((block, per, width), jnp.float32),
        grid=(block // tile,),
        in_specs=[spec] * (per + 1),
        out_specs=pl.BlockSpec((tile, per, width), lambda i: (i, 0, 0)),
        cost_estimate=pl.CostEstimate(
            flops=block * width, bytes_accessed=4 * block * width * (2 * per + 1), transcendentals=0
        ),
        name="weave",
    )(*done, fresh, away)


def share(rows):
    experts, hid = lax.axis_size("expert"), lax.axis_size("hid")
    if experts != 4 or hid != 2:
        rows = lax.all_gather(rows, ("expert", "hid"), axis=0, tiled=False)
        return rows.reshape(experts, hid, *rows.shape[1:])
    me, h = lax.axis_index("expert"), lax.axis_index("hid")

    def hop(value, bit):
        return lax.ppermute(value, "expert", [(p, p ^ bit) for p in range(experts)])

    def across(value):
        return lax.ppermute(value, "hid", [(0, 1), (1, 0)])

    parts = [rows] + [hop(rows, bit) for bit in range(1, experts)]
    result = jnp.zeros((experts, hid, *rows.shape), rows.dtype)
    for bit, value in enumerate(parts):
        for side, block in ((h, value), (1 - h, across(value))):
            start = (me ^ bit, side) + (0,) * rows.ndim
            result = lax.dynamic_update_slice(result, block[None, None], start)
    return result


def shards(calib_rows, routes, sketch_seed, up_weight):
    per, local, full = up_weight.shape
    tokens = calib_rows.shape[0]
    width = sketch_seed.shape[1]
    hid = lax.axis_size("hid")
    chips = lax.axis_size("rep") * lax.axis_size("expert")
    d = local // chips
    h = lax.axis_index("hid")

    ids = jnp.arange(EXPERTS, dtype=jnp.int32)
    member = jnp.sum((routes.T[:, None, :] == ids[None, :, None]).astype(jnp.float32), axis=0)
    row_squares = jnp.sum(jnp.square(calib_rows.astype(jnp.float32)), axis=1)
    squares = split3(jnp.sum(member * row_squares[None, :], axis=1))
    extra = jnp.zeros((EXTRA, tokens), jnp.float32)
    extra = extra.at[:EXPERTS].set(member)
    extra = extra.at[EXPERTS : EXPERTS + 3, :EXPERTS].set(squares).astype(jnp.bfloat16)
    pieces = flip(calib_rows, extra, chips)
    received = lax.all_to_all(pieces, ("rep", "expert"), split_axis=0, concat_axis=0, tiled=True)
    part = jnp.dot(calib_rows, sketch_seed.astype(jnp.bfloat16), preferred_element_type=jnp.float32)
    if hid == 2:
        half = tokens // 2
        mine = lax.dynamic_slice_in_dim(part, h * half, half) + lax.ppermute(
            lax.dynamic_slice_in_dim(part, (1 - h) * half, half), "hid", [(0, 1), (1, 0)]
        )
    else:
        mine = lax.psum_scatter(part, "hid", scatter_dimension=0, tiled=True)
    sketched = lax.all_gather(mine.astype(jnp.bfloat16), "rep", axis=0, tiled=False)
    sketched = share(sketched)

    stats = received[:, d:, :].astype(jnp.float32)
    counts = jnp.sum(stats[:, :EXPERTS], axis=(0, 2))
    square_sums = lax.psum(jnp.sum(stats[:, EXPERTS : EXPERTS + 3, :EXPERTS], axis=(0, 1)), "hid")
    ridge = damping * square_sums / (counts * D)
    place = lax.axis_index(("rep", "expert"))
    signs = lax.dynamic_slice_in_dim(sketch_seed, place * d, d, 0)

    block = full // hid
    swap = [(0, 1), (1, 0)]
    outs, owns = [], []
    for k in range(per):
        own = gram(counts, ridge, received, sketched, signs, k, per)
        own = lax.all_to_all(own, "expert", split_axis=0, concat_axis=0, tiled=True)
        owns.append(own.reshape(-1, width))
    sketches = []
    for k, own in enumerate(owns):
        sketches.append(lax.all_gather(own, "rep", axis=0, tiled=True))
    for k in range(per):
        sketch = lax.optimization_barrier((sketches[k], owns))[0]

        def project(start, size):
            weight = lax.dynamic_slice(up_weight, (k, 0, start), (1, local, size))[0]
            return lax.dot_general(
                weight, sketch, (((0,), (0,)), ((), ())), preferred_element_type=jnp.float32
            )

        if hid != 2:
            outs.append(
                lax.psum_scatter(project(0, full), "hid", scatter_dimension=0, tiled=True)
            )
            continue
        if outs:
            sketch, outs = lax.optimization_barrier((sketch, outs))
        away = lax.ppermute(project((1 - h) * block, block), "hid", swap)
        if k == per - 1:
            return weave(outs, project(h * block, block), away)
        outs.append(project(h * block, block) + away)
    return jnp.stack(outs, axis=1)


def solution(mesh):
    in_specs = (
        P(("expert", "rep"), "hid"),
        P(("expert", "rep"), None),
        P("hid", None),
        P("expert", "hid", "rep"),
    )
    out_specs = P(("rep", "hid"), "expert", None)

    return jax.shard_map(shards, mesh=mesh, in_specs=in_specs, out_specs=out_specs, check_vma=False)
```

```python
import math

import jax
import jax.numpy as jnp
from jax import lax
from jax.experimental import pallas as pl
from jax.experimental.pallas import tpu as pltpu
from jax.sharding import PartitionSpec as P


D = 6144
EXPERTS = 8
EXTRA = 16
damping = 0.25


def split3(value):
    hi = lax.reduce_precision(value, 8, 7)
    mid = lax.reduce_precision(value - hi, 8, 7)
    return jnp.stack([hi, mid, value - hi - mid])


def flip_kernel(x_ref, extra_ref, p_ref, *, d):
    flipped = x_ref[...].T
    for g in range(p_ref.shape[0]):
        p_ref[g, :d, :] = flipped[g * d : (g + 1) * d, :]
        p_ref[g, d:, :] = extra_ref[...]


def flip(calib_rows, extra, chips):
    tokens, local = calib_rows.shape
    d = local // chips
    group = 128 // math.gcd(d, 128)
    if d % 16 or chips % group:
        return jnp.concatenate(
            [
                calib_rows.T.reshape(chips, d, tokens),
                jnp.broadcast_to(extra[None], (chips, EXTRA, tokens)),
            ],
            axis=1,
        )
    return pl.pallas_call(
        lambda *refs: flip_kernel(*refs, d=d),
        out_shape=jax.ShapeDtypeStruct((chips, d + EXTRA, tokens), jnp.bfloat16),
        grid=(chips // group,),
        in_specs=[
            pl.BlockSpec((tokens, group * d), lambda j: (0, j)),
            pl.BlockSpec((EXTRA, tokens), lambda j: (0, 0)),
        ],
        out_specs=pl.BlockSpec((group, d + EXTRA, tokens), lambda j: (j, 0, 0)),
        cost_estimate=pl.CostEstimate(
            flops=tokens * local, bytes_accessed=4 * tokens * local, transcendentals=0
        ),
        name="flip",
    )(calib_rows, extra)


def gram_kernel(counts_ref, ridge_ref, at_ref, x_ref, s_ref, *rest, which, per, d):
    m_refs, (o_ref, lhs, acc, right) = rest[:-4], rest[-4:]
    step = pl.program_id(0)
    groups = o_ref.shape[0]
    sources, _, tokens = x_ref.shape
    for s in range(sources):
        x = x_ref[s, :d, :]
        for g in range(groups):
            row = d + g * per + which
            lhs[g, :, s * tokens : (s + 1) * tokens] = x * x_ref[s, row : row + 1, :]
    flat = lhs[...].reshape(groups * d, sources * tokens)
    if len(m_refs) == 1:
        right[...] = m_refs[0][...].reshape(right.shape)
    else:
        me, h = at_ref[0], at_ref[1]
        half = tokens // 2
        for i, m_ref in enumerate(m_refs):
            side = h if i % 2 == 0 else 1 - h
            row = pl.multiple_of(((me ^ (i // 2)) * 2 + side) * half, half)
            right[pl.ds(row, half), :] = m_ref[0]
    part = jnp.dot(flat, right[...], preferred_element_type=jnp.float32)

    @pl.when(step == 0)
    def _():
        acc[...] = part

    @pl.when(step > 0)
    def _():
        acc[...] += part

    @pl.when(step == pl.num_programs(0) - 1)
    def _():
        signs = s_ref[...].astype(jnp.float32)
        for g in range(groups):
            e = g * per + which
            total = acc[g * d : (g + 1) * d, :]
            o_ref[g] = (total / counts_ref[e] + ridge_ref[e] * signs).astype(jnp.bfloat16)


def gram(counts, ridge, at, received, sketched, signs, which, per):
    sources, rows, tokens = received.shape
    d = rows - EXTRA
    width = signs.shape[1]
    if isinstance(sketched, list):
        batch = len(sketched) // 2
        m_specs = [pl.BlockSpec((1, tokens // 2, width), lambda j: (j, 0, 0))] * len(sketched)
    else:
        batch, hid, _, part = sketched.shape[:4]
        m_specs = [pl.BlockSpec((batch, hid, 1, part, width), lambda j: (0, 0, j, 0, 0))]
        sketched = [sketched]
    groups = EXPERTS // per
    return pl.pallas_call(
        lambda *refs: gram_kernel(*refs, which=which, per=per, d=d),
        out_shape=jax.ShapeDtypeStruct((groups, d, width), jnp.bfloat16),
        grid=(sources // batch,),
        in_specs=[
            pl.BlockSpec(memory_space=pltpu.SMEM),
            pl.BlockSpec(memory_space=pltpu.SMEM),
            pl.BlockSpec(memory_space=pltpu.SMEM),
            pl.BlockSpec((batch, rows, tokens), lambda j: (j, 0, 0)),
            pl.BlockSpec((d, width), lambda j: (0, 0)),
            *m_specs,
        ],
        out_specs=pl.BlockSpec((groups, d, width), lambda j: (0, 0, 0)),
        scratch_shapes=[
            pltpu.VMEM((groups, d, batch * tokens), jnp.bfloat16),
            pltpu.VMEM((groups * d, width), jnp.float32),
            pltpu.VMEM((batch * tokens, width), jnp.bfloat16),
        ],
        cost_estimate=pl.CostEstimate(
            flops=2 * sources * groups * d * tokens * width,
            bytes_accessed=2 * sources * tokens * (rows + width),
            transcendentals=0,
        ),
        name="gram",
    )(counts, ridge, at, received, signs, *sketched)


def weave_kernel(*refs, fresh):
    away_ref, o_ref = refs[-2:]
    for k, ref in enumerate(refs[:-2]):
        value = ref[...]
        o_ref[:, k, :] = value + away_ref[...] if k == fresh else value


def weave(parts, fresh, away):
    block, width = away.shape
    per = len(parts)
    tile = math.gcd(block, 256)
    spec = pl.BlockSpec((tile, width), lambda i: (i, 0))
    return pl.pallas_call(
        lambda *refs: weave_kernel(*refs, fresh=fresh),
        out_shape=jax.ShapeDtypeStruct((block, per, width), jnp.float32),
        grid=(block // tile,),
        in_specs=[spec] * (per + 1),
        out_specs=pl.BlockSpec((tile, per, width), lambda i: (i, 0, 0)),
        cost_estimate=pl.CostEstimate(
            flops=block * width, bytes_accessed=4 * block * width * (2 * per + 1), transcendentals=0
        ),
        name="weave",
    )(*parts, away)


def share(rows):
    experts, hid = lax.axis_size("expert"), lax.axis_size("hid")
    if experts != 4 or hid != 2:
        rows = lax.all_gather(rows, ("expert", "hid"), axis=0, tiled=False)
        return rows.reshape(experts, hid, *rows.shape[1:])

    def hop(value, bit):
        return lax.ppermute(value, "expert", [(p, p ^ bit) for p in range(experts)])

    def across(value):
        return lax.ppermute(value, "hid", [(0, 1), (1, 0)])

    half = rows.shape[0] // 2
    one, two = hop(rows, 1), hop(rows, 2)
    both = [hop(two[:half], 1), hop(one[half:], 2)]
    both = jnp.concatenate(both, axis=0)
    blocks = []
    for value in (rows, one, two, both):
        blocks += [value, across(value)]
    return blocks


def ring(own, others):
    size, me = lax.axis_size("rep"), lax.axis_index("rep")
    right, left, ups, downs = own, own, [], []
    for step in range(1, size):
        ups_pairs = [(p, p + 1) for p in range(step - 1, size - 1)]
        down_pairs = [(p + 1, p) for p in range(size - step)]
        right = lax.ppermute(right, "rep", ups_pairs)
        left = lax.ppermute(left, "rep", down_pairs)
        if step == 1:
            right, left = lax.optimization_barrier((right, left, others))[:2]
        ups.append(right)
        downs.append(left)
    result = jnp.zeros((size, *own.shape), own.dtype)
    result = lax.dynamic_update_slice(result, own[None], (me, 0, 0))
    for step in range(1, size):
        block = jnp.where(me >= step, ups[step - 1], downs[size - 1 - step])
        start = ((me - step) % size, 0, 0)
        result = lax.dynamic_update_slice(result, block[None], start)
    return result.reshape(size * own.shape[0], own.shape[1])


def shards(calib_rows, routes, sketch_seed, up_weight):
    per, local, full = up_weight.shape
    tokens = calib_rows.shape[0]
    width = sketch_seed.shape[1]
    hid = lax.axis_size("hid")
    chips = lax.axis_size("rep") * lax.axis_size("expert")
    d = local // chips
    h = lax.axis_index("hid")

    ids = jnp.arange(EXPERTS, dtype=jnp.int32)
    member = jnp.sum((routes.T[:, None, :] == ids[None, :, None]).astype(jnp.float32), axis=0)
    row_squares = jnp.sum(jnp.square(calib_rows.astype(jnp.float32)), axis=1)
    squares = split3(jnp.sum(member * row_squares[None, :], axis=1))
    extra = jnp.zeros((EXTRA, tokens), jnp.float32)
    extra = extra.at[:EXPERTS].set(member)
    extra = extra.at[EXPERTS : EXPERTS + 3, :EXPERTS].set(squares).astype(jnp.bfloat16)
    pieces = flip(calib_rows, extra, chips)
    received = lax.all_to_all(pieces, ("rep", "expert"), split_axis=0, concat_axis=0, tiled=True)
    part = jnp.dot(calib_rows, sketch_seed.astype(jnp.bfloat16), preferred_element_type=jnp.float32)
    if hid == 2:
        half = tokens // 2
        mine = lax.dynamic_slice_in_dim(part, h * half, half) + lax.ppermute(
            lax.dynamic_slice_in_dim(part, (1 - h) * half, half), "hid", [(0, 1), (1, 0)]
        )
    else:
        mine = lax.psum_scatter(part, "hid", scatter_dimension=0, tiled=True)
    sketched = lax.all_gather(mine.astype(jnp.bfloat16), "rep", axis=0, tiled=False)
    sketched = share(sketched)

    stats = received[:, d:, :].astype(jnp.float32)
    counts = jnp.sum(stats[:, :EXPERTS], axis=(0, 2))
    square_sums = lax.psum(jnp.sum(stats[:, EXPERTS : EXPERTS + 3, :EXPERTS], axis=(0, 1)), "hid")
    ridge = damping * square_sums / (counts * D)
    place = lax.axis_index(("rep", "expert"))
    at = jnp.stack([lax.axis_index("expert"), h]).astype(jnp.int32)
    signs = lax.dynamic_slice_in_dim(sketch_seed, place * d, d, 0)

    block = full // hid
    swap = [(0, 1), (1, 0)]
    owns = []
    for k in range(per):
        own = gram(counts, ridge, at, received, sketched, signs, k, per)
        own = lax.all_to_all(own, "expert", split_axis=0, concat_axis=0, tiled=True)
        owns.append(own.reshape(-1, width))
    sketches = []
    for k, own in enumerate(owns):
        if hid == 2 and k == per - 1:
            sketches.append(ring(own, owns[:k]))
        else:
            sketches.append(lax.all_gather(own, "rep", axis=0, tiled=True))
    outs = [None] * per
    for turn, k in enumerate(reversed(range(per))):
        sketch = lax.optimization_barrier((sketches[k], owns))[0]

        def project(start, size):
            weight = lax.dynamic_slice(up_weight, (k, 0, start), (1, local, size))[0]
            return lax.dot_general(
                weight, sketch, (((0,), (0,)), ((), ())), preferred_element_type=jnp.float32
            )

        if hid != 2:
            outs[k] = lax.psum_scatter(project(0, full), "hid", scatter_dimension=0, tiled=True)
            continue
        if turn:
            sketch, outs[k + 1] = lax.optimization_barrier((sketch, outs[k + 1]))
        away = lax.ppermute(project((1 - h) * block, block), "hid", swap)
        if turn == per - 1:
            outs[k] = project(h * block, block)
            return weave(outs, k, away)
        outs[k] = project(h * block, block) + away
    return jnp.stack(outs, axis=1)


def solution(mesh):
    in_specs = (
        P(("expert", "rep"), "hid"),
        P(("expert", "rep"), None),
        P("hid", None),
        P("expert", "hid", "rep"),
    )
    out_specs = P(("rep", "hid"), "expert", None)

    return jax.shard_map(shards, mesh=mesh, in_specs=in_specs, out_specs=out_specs, check_vma=False)
```
